32 devices in a mesh: group: 2 (over y), blk: 4 (over z), uly: 4 (over x, core).
Axes of the slice: x: 2, y: 2, z: 4, core: 2. Of those that a mesh axis runs over, the one named last changes fastest.
Arguments:
- query: bfloat16 [768, 3072], P(('group', 'blk', 'uly')), parts along dimension 0, may hold values from -16 to 16
- keys: bfloat16 [768, 3072], P(('group', 'blk', 'uly')), parts along dimension 0, may hold values from -16 to 16
- values: bfloat16 [768, 3072], P(('group', 'blk', 'uly')), parts along dimension 0, may hold values from -6 to 6
- out_weight: bfloat16 [3072, 3072], P('uly', 'blk'), may hold values from -1 to 1
- out_gain: float32 [3072], replicated, may hold values from 0.1 to 1.9
Outputs:
- gated_out: bfloat16 [768, 3072], P(('group', 'blk', 'uly')), parts along dimension 0
The draws below stay inside these ranges and needn't reach their ends.
There are 2 independent parts, one for each index of `group`. The reference program is written for one: setup_inputs(seed, part) draws one part's arguments, and reference() takes and returns one part's arrays. A program takes and returns all parts, laid end to end along the dimension named above; an argument that names none is the same for every part. Nothing has to cross between parts.
All inputs are finite; a program needn't handle non-finite values.
Results may differ from the reference program's by a relative error of at most 0.015.
Values may be sent and summed in bfloat16 or wider, within the bound.
A program may use at most 128 MiB of HBM per device.

```python
import math
import jax
import jax.numpy as jnp
from jax import lax

D = 3072
H = 48
HEAD = 64
TOKENS = 384


def pair_draw(key):
    key_query, key_keys = jax.random.split(jax.random.fold_in(key, 7013), 2)
    query = jnp.clip(1.4 * jax.random.normal(key_query, (TOKENS, D), jnp.float32), -8.0, 8.0)
    keys = jnp.clip(1.4 * jax.random.normal(key_keys, (TOKENS, D), jnp.float32), -8.0, 8.0)
    return (query, keys)


def draw_query(key, part):
    return pair_draw(key)[0].astype(jnp.bfloat16)


def draw_keys(key, part):
    return pair_draw(key)[1].astype(jnp.bfloat16)


def level_of(rng, shape, pieces, smallest, high):
    gain, own = 1.0, jax.random.fold_in(rng, 6)
    for axis_at, shards_of in pieces:
        heights = jnp.exp(jax.random.uniform(jax.random.fold_in(own, axis_at), (shards_of,), jnp.float32, smallest / len(pieces), high / len(pieces)))
        gain = gain * jnp.repeat(heights, shape[axis_at] // shards_of).reshape([-1 if axis == axis_at else 1 for axis in range(len(shape))])
    return gain


def scatter_about(key, shape, deviation, bound, cuts=(), held_as=jnp.bfloat16):
    drawn = jax.random.normal(key, shape, jnp.float32) * deviation
    if len(cuts) > 0:
        drawn = level_of(key, shape, cuts, -0.22, 0.18) * drawn
    return jnp.clip(drawn, min=-bound, max=bound).astype(held_as)


def setup_inputs(seed: int = 0, part: int = 0) -> dict:
    arg_keys = jax.random.split(jax.random.key(seed), 6)
    own_keys = jax.random.split(jax.random.fold_in(arg_keys[5], part), 6)
    query = draw_query(jax.random.fold_in(jax.random.fold_in(arg_keys[5], part), 71), part)
    keys = draw_keys(jax.random.fold_in(jax.random.fold_in(arg_keys[5], part), 71), part)
    values = scatter_about(own_keys[2], (TOKENS, D), 1.0, 6.0, ((0, 16),))
    out_weight = scatter_about(arg_keys[3], (D, D), (HEAD // 2) ** -0.5, 1.0, ((0, 4), (1, 4)))
    out_gain = jnp.clip(1.0 + 0.18 * jax.random.normal(arg_keys[4], (D,), jnp.float32), 0.1, 1.9)
    return {"query": query, "keys": keys, "values": values, "out_weight": out_weight, "out_gain": out_gain}


def reference(query, keys, values, out_weight, out_gain):
    score_scale = 1.0 / math.sqrt(HEAD)
    query_heads = query.reshape(TOKENS, H, HEAD).transpose(1, 0, 2)
    key_heads = keys.reshape(TOKENS, H, HEAD).transpose(1, 0, 2)
    value_heads = values.reshape(TOKENS, H, HEAD).transpose(1, 0, 2)

    def attend(triple):
        query_one, key_one, value_one = triple
        scores = jnp.dot(query_one, key_one.T, preferred_element_type=jnp.float32) * score_scale
        row_max = lax.optimization_barrier(jnp.max(scores, axis=1, keepdims=True))
        weights = jnp.exp(scores - row_max)
        denominator = lax.optimization_barrier(jnp.sum(weights, axis=1, keepdims=True))
        return jnp.dot(weights.astype(jnp.bfloat16), value_one, preferred_element_type=jnp.float32) / denominator
    per_head = lax.map(attend, (query_heads, key_heads, value_heads))
    attended = per_head.transpose(1, 0, 2).reshape(TOKENS, D).astype(jnp.bfloat16)
    projected = jnp.dot(attended, out_weight, preferred_element_type=jnp.float32)
    return (out_gain * projected).astype(jnp.bfloat16)
```

```python
import functools
import math

import jax
import jax.numpy as jnp
from jax import lax
from jax.experimental import pallas as pl
from jax.experimental.pallas import tpu as pltpu
from jax.sharding import PartitionSpec as P

HEAD = 64
LANES = 128
MESH = pl.DeviceIdType.MESH

def make_fold(query_heads, state_now, pieces):
    score_scale = 1.0 / math.sqrt(HEAD)
    head_count = query_heads.shape[1]
    running_max, denominator, weighted = state_now
    key_part, value_part = pieces
    key_count = key_part.shape[0]
    key_heads = key_part.reshape(key_count, head_count, HEAD)
    value_heads = value_part.reshape(key_count, head_count, HEAD)
    scores = (
        jnp.einsum("qhd,khd->qhk", query_heads, key_heads, preferred_element_type=jnp.float32)
        * score_scale
    )
    new_max = jnp.max(scores, axis=2)
    weights = jnp.exp(scores - new_max[:, :, None])
    shrink = jnp.exp(running_max - new_max)
    denominator = denominator * shrink + jnp.sum(weights, axis=2)
    weighted = weighted * shrink[:, :, None] + jnp.einsum(
        "qhk,khd->qhd",
        weights.astype(jnp.bfloat16),
        value_heads,
        preferred_element_type=jnp.float32,
    )
    return (new_max, denominator, weighted)


def initial_state(row_count, head_count):
    return (
        jnp.full((row_count, head_count), -jnp.inf, jnp.float32),
        jnp.zeros((row_count, head_count), jnp.float32),
        jnp.zeros((row_count, head_count, HEAD), jnp.float32),
    )


def on_device(query, keys, values, out_weight, out_gain):
    grouped_q, grouped_k, grouped_v = (
        lax.all_to_all(query, "uly", split_axis=1, concat_axis=0, tiled=True),
        lax.all_to_all(keys, "uly", split_axis=1, concat_axis=0, tiled=True),
        lax.all_to_all(values, "uly", split_axis=1, concat_axis=0, tiled=True),
    )
    row_count = grouped_q.shape[0]
    features = grouped_q.shape[1]
    local_heads = features // HEAD
    query_heads = grouped_q.reshape(row_count, local_heads, HEAD)
    half_heads = local_heads // 2
    half_width = half_heads * HEAD
    low_state = make_fold(
        query_heads[:, :half_heads],
        initial_state(row_count, half_heads),
        (
            lax.all_gather(grouped_k[:, :half_width], "blk", axis=0, tiled=True),
            lax.all_gather(grouped_v[:, :half_width], "blk", axis=0, tiled=True),
        ),
    )
    high_state = make_fold(
        query_heads[:, half_heads:],
        initial_state(row_count, local_heads - half_heads),
        (
            lax.all_gather(grouped_k[:, half_width:], "blk", axis=0, tiled=True),
            lax.all_gather(grouped_v[:, half_width:], "blk", axis=0, tiled=True),
        ),
    )
    denominator = jnp.concatenate([low_state[1], high_state[1]], axis=1)
    weighted = jnp.concatenate([low_state[2], high_state[2]], axis=1)
    attended = (
        (weighted / denominator[:, :, None]).reshape(row_count, features).astype(jnp.bfloat16)
    )
    partial_value = jnp.dot(
        attended,
        lax.all_gather(out_weight, "blk", axis=1, tiled=True),
        preferred_element_type=jnp.float32,
    )
    summed = lax.psum_scatter(
        partial_value.astype(jnp.bfloat16), "uly", scatter_dimension=0, tiled=True
    ).astype(jnp.float32)
    return (out_gain * summed).astype(jnp.bfloat16)


def attend_kernel(
    nb, nu,
    q_ref, k_ref, v_ref, w_hbm, gain_ref, out_ref,
    stage_a, stage_b, got_a, got_b, w_ref,
    att_pair, att_one, att_all, part_f32, part_send, part_got, final_send,
    w_sem, send_a, send_b, recv_a, recv_b,
    send_p, recv_p, send_o, recv_o, send_r, recv_r, send_f, recv_f,
):
    n = nb * nu
    rows, width = q_ref.shape
    tokens = n * rows
    pairs = stage_a.shape[1] // 3
    heads = 2 * pairs + 1
    half = tokens // 2
    block = nu * rows
    scale = 1.0 / math.sqrt(HEAD)
    me_b, me_u = lax.axis_index("blk"), lax.axis_index("uly")
    me = me_b * nu + me_u

    def there(b, u):
        return dict(device_id={"blk": b, "uly": u}, device_id_type=MESH)

    barrier = pltpu.get_barrier_semaphore()

    @pl.loop(1, n)
    def _(d):
        j = lax.rem(me + d, n)
        pl.semaphore_signal(barrier, inc=1, **there(j // nu, lax.rem(j, nu)))

    w_copy = pltpu.make_async_copy(w_hbm, w_ref, w_sem)
    w_copy.start()

    lane = lax.broadcasted_iota(jnp.int32, (rows, LANES), 1)
    low = lane < HEAD
    for c in range(n):
        odd = c % 2
        first = (heads * c - odd) // 2
        pair_at = first + odd
        one_at = first + (0 if odd else pairs)
        for s, ref in enumerate((q_ref, k_ref, v_ref)):
            for p in range(pairs):
                stage_a[c, s * pairs + p] = ref[:, pl.ds((pair_at + p) * LANES, LANES)]
        q_tile = q_ref[:, pl.ds(one_at * LANES, LANES)]
        k_tile = k_ref[:, pl.ds(one_at * LANES, LANES)]
        if odd:
            stage_b[c, 0] = jnp.concatenate([q_tile[:, HEAD:], k_tile[:, HEAD:]], axis=1)
        else:
            stage_b[c, 0] = jnp.concatenate([q_tile[:, :HEAD], k_tile[:, :HEAD]], axis=1)
        stage_b[c, 1] = v_ref[:, pl.ds(one_at * LANES, LANES)]
    mine = me_u * nb + me_b
    got_a[me] = stage_a[mine]
    got_b[me] = stage_b[mine]

    pl.semaphore_wait(barrier, n - 1)

    def exchange(stage, got, send, recv, d):
        j = lax.rem(me + d, n)
        b, u = j // nu, lax.rem(j, nu)
        return pltpu.make_async_remote_copy(
            src_ref=stage.at[u * nb + b], dst_ref=got.at[me],
            send_sem=send.at[d], recv_sem=recv.at[me], **there(b, u))

    def arrival(stage, got, send, recv, d):
        j = lax.rem(me + n - d, n)
        return pltpu.make_async_remote_copy(
            src_ref=stage.at[j], dst_ref=got.at[j],
            send_sem=send.at[d], recv_sem=recv.at[j], **there(me_b, me_u))

    a_refs = (stage_a, got_a, send_a, recv_a)
    b_refs = (stage_b, got_b, send_b, recv_b)

    @pl.loop(1, n)
    def _(d):
        exchange(*a_refs, d).start()

    @pl.loop(1, n)
    def _(d):
        exchange(*b_refs, d).start()

    @pl.loop(1, n)
    def _(d):
        arrival(*a_refs, d).wait_recv()

    def softmax(scores):
        scores = scores * scale
        top = jnp.max(scores, axis=1, keepdims=True)
        weights = jnp.exp(scores - top)
        return weights.astype(jnp.bfloat16), jnp.sum(weights, axis=1, keepdims=True)

    def against(a, b):
        return lax.dot_general(a, b, (((1,), (1,)), ((), ())), preferred_element_type=jnp.float32)

    wide_low = lax.broadcasted_iota(jnp.int32, (tokens, LANES), 1) < HEAD

    def whole(ref, s):
        return jnp.concatenate([ref[i, s].astype(jnp.float32) for i in range(n)], axis=0)

    for p in range(pairs):
        q_all = whole(got_a, p)
        k_all = whole(got_a, pairs + p).astype(jnp.bfloat16)
        v_all = whole(got_a, 2 * pairs + p).astype(jnp.bfloat16)
        pieces = []
        for keep in (wide_low, jnp.logical_not(wide_low)):
            q_one = jnp.where(keep, q_all, 0.0).astype(jnp.bfloat16)
            weights, total = softmax(against(q_one, k_all))
            pieces.append(jnp.dot(weights, v_all, preferred_element_type=jnp.float32) / total)
        att_pair[me_b, p] = jnp.where(wide_low, *pieces).astype(jnp.bfloat16)

    def spread(ref, send, recv, d):
        b = lax.rem(me_b + d, nb)
        return pltpu.make_async_remote_copy(
            src_ref=ref.at[me_b], dst_ref=ref.at[me_b],
            send_sem=send.at[d], recv_sem=recv.at[me_b], **there(b, me_u))

    def spread_in(ref, send, recv, d):
        b = lax.rem(me_b + nb - d, nb)
        return pltpu.make_async_remote_copy(
            src_ref=ref.at[b], dst_ref=ref.at[b],
            send_sem=send.at[d], recv_sem=recv.at[b], **there(me_b, me_u))

    for d in range(1, nb):
        spread(att_pair, send_p, recv_p, d).start()

    @pl.loop(1, n)
    def _(d):
        arrival(*b_refs, d).wait_recv()

    qk_all = whole(got_b, 0)
    v_all = whole(got_b, 1).astype(jnp.bfloat16)
    weights, total = softmax(
        against(qk_all[:, :HEAD].astype(jnp.bfloat16), qk_all[:, HEAD:].astype(jnp.bfloat16)))
    wide = jnp.dot(weights, v_all, preferred_element_type=jnp.float32) / total
    single = jnp.where(lax.rem(me_b, 2) == 0, wide[:, :HEAD], wide[:, HEAD:])
    att_one[me_b] = jnp.concatenate([single[:half], single[half:]], axis=1).astype(jnp.bfloat16)
    for d in range(1, nb):
        spread(att_one, send_o, recv_o, d).start()

    w_copy.wait()
    for d in range(1, nb):
        spread_in(att_pair, send_p, recv_p, d).wait_recv()
    for b in range(nb):
        odd = b % 2
        first = (heads * b - odd) // 2 + odd
        for p in range(pairs):
            att_all[:, pl.ds((first + p) * LANES, LANES)] = att_pair[b, p]
    for d in range(1, nb):
        spread_in(att_one, send_o, recv_o, d).wait_recv()
    for b in range(0, nb, 2):
        even, odd = att_one[b], att_one[b + 1]
        at = pl.ds((heads * b // 2 + pairs) * LANES, LANES)
        att_all[:half, at] = jnp.concatenate([even[:, :HEAD], odd[:, :HEAD]], axis=1)
        att_all[half:, at] = jnp.concatenate([even[:, HEAD:], odd[:, HEAD:]], axis=1)

    def scatter(to, d):
        u = lax.rem(me_u + d, nu)
        return pltpu.make_async_remote_copy(
            src_ref=part_send.at[to, u], dst_ref=part_got.at[to, me_u],
            send_sem=send_r.at[to, d], recv_sem=recv_r.at[to, me_u], **there(me_b, u))

    def scatter_in(to, d):
        u = lax.rem(me_u + nu - d, nu)
        return pltpu.make_async_remote_copy(
            src_ref=part_send.at[to, u], dst_ref=part_got.at[to, u],
            send_sem=send_r.at[to, d], recv_sem=recv_r.at[to, u], **there(me_b, me_u))

    def final(d):
        to = lax.rem(me_b + d, nb)
        return pltpu.make_async_remote_copy(
            src_ref=final_send.at[to], dst_ref=out_ref.at[me_b],
            send_sem=send_f.at[d], recv_sem=recv_f.at[me_b], **there(to, me_u))

    def final_in(d):
        b = lax.rem(me_b + nb - d, nb)
        return pltpu.make_async_remote_copy(
            src_ref=final_send.at[b], dst_ref=out_ref.at[b],
            send_sem=send_f.at[d], recv_sem=recv_f.at[b], **there(me_b, me_u))

    for e in range(1, nb + 1):
        to = lax.rem(me_b + e, nb)
        part = jnp.dot(
            att_all[pl.ds(pl.multiple_of(to * block, block), block), :], w_ref[...],
            preferred_element_type=jnp.float32)
        for u in range(nu):
            one = part[u * rows:(u + 1) * rows]
            part_f32[to, u] = one
            part_send[to, u] = one.astype(jnp.bfloat16)
        for d in range(1, nu):
            scatter(to, d).start()

    for e in range(1, nb + 1):
        to = lax.rem(me_b + e, nb)
        total = part_f32[to, me_u]
        for d in range(1, nu):
            scatter_in(to, d).wait_recv()
            total += part_got[to, lax.rem(me_u + nu - d, nu)].astype(jnp.float32)
        gated = (gain_ref[me_b] * total).astype(jnp.bfloat16)
        if e < nb:
            final_send[to] = gated
            final(e).start()
        else:
            out_ref[me_b] = gated

    for d in range(1, nb):
        final_in(d).wait_recv()

    @pl.loop(1, n)
    def _(d):
        exchange(*a_refs, d).wait_send()
        exchange(*b_refs, d).wait_send()

    for d in range(1, nb):
        spread(att_pair, send_p, recv_p, d).wait_send()
        spread(att_one, send_o, recv_o, d).wait_send()
        final(d).wait_send()
    for e in range(1, nb + 1):
        to = lax.rem(me_b + e, nb)
        for d in range(1, nu):
            scatter(to, d).wait_send()


def fused(nb, nu, query, keys, values, out_weight, out_gain):
    n = nb * nu
    rows, width = query.shape
    heads = width // HEAD // n
    pairs = heads // 2
    depth, columns = out_weight.shape
    tokens = n * rows
    bf16, f32 = jnp.bfloat16, jnp.float32
    vmem, dma = pltpu.VMEM, pltpu.SemaphoreType.DMA
    in_vmem = pl.BlockSpec(memory_space=pltpu.VMEM)
    gathered = pl.pallas_call(
        functools.partial(attend_kernel, nb, nu),
        out_shape=jax.ShapeDtypeStruct((nb, rows, columns), bf16),
        in_specs=[in_vmem, in_vmem, in_vmem, pl.BlockSpec(memory_space=pl.ANY), in_vmem],
        out_specs=in_vmem,
        scratch_shapes=[
            vmem((n, 3 * pairs, rows, LANES), bf16),
            vmem((n, 2, rows, LANES), bf16),
            vmem((n, 3 * pairs, rows, LANES), bf16),
            vmem((n, 2, rows, LANES), bf16),
            vmem((depth, columns), bf16),
            vmem((nb, pairs, tokens, LANES), bf16),
            vmem((nb, tokens // 2, LANES), bf16),
            vmem((tokens, depth), bf16),
            vmem((nb, nu, rows, columns), f32),
            vmem((nb, nu, rows, columns), bf16),
            vmem((nb, nu, rows, columns), bf16),
            vmem((nb, rows, columns), bf16),
            dma, dma((n,)), dma((n,)), dma((n,)), dma((n,)),
            dma((nb,)), dma((nb,)), dma((nb,)), dma((nb,)),
            dma((nb, nu)), dma((nb, nu)), dma((nb,)), dma((nb,)),
        ],
        compiler_params=pltpu.CompilerParams(collective_id=0, has_side_effects=True),
    )(query, keys, values, out_weight, out_gain.reshape(nb, 1, columns))
    return gathered.transpose(1, 0, 2).reshape(rows, width)


def on_any(nb, nu, query, keys, values, out_weight, out_gain):
    n = nb * nu
    rows, width = query.shape
    heads = width // HEAD
    suits = (
        heads % n == 0 and (heads // n) % 2 == 1 and heads // n > 1 and nb % 2 == 0
        and rows % 8 == 0 and (width // nb) % LANES == 0
    )
    plan = functools.partial(fused, nb, nu) if suits else on_device
    return plan(query, keys, values, out_weight, out_gain)


def solution(mesh):
    in_specs = (
        P(("group", "blk", "uly"), None),
        P(("group", "blk", "uly"), None),
        P(("group", "blk", "uly"), None),
        P("uly", "blk"),
        P(),
    )
    out_specs = P(("group", "blk", "uly"), None)
    body = functools.partial(on_any, mesh.shape["blk"], mesh.shape["uly"])
    return jax.shard_map(
        body, mesh=mesh, in_specs=in_specs, out_specs=out_specs, check_vma=False
    )
```

```python
import functools
import math

import jax
import jax.numpy as jnp
from jax import lax
from jax.experimental import pallas as pl
from jax.experimental.pallas import tpu as pltpu
from jax.sharding import PartitionSpec as P

HEAD = 64
LANES = 128
MESH = pl.DeviceIdType.MESH

def make_fold(query_heads, state_now, pieces):
    score_scale = 1.0 / math.sqrt(HEAD)
    head_count = query_heads.shape[1]
    running_max, denominator, weighted = state_now
    key_part, value_part = pieces
    key_count = key_part.shape[0]
    key_heads = key_part.reshape(key_count, head_count, HEAD)
    value_heads = value_part.reshape(key_count, head_count, HEAD)
    scores = (
        jnp.einsum("qhd,khd->qhk", query_heads, key_heads, preferred_element_type=jnp.float32)
        * score_scale
    )
    new_max = jnp.max(scores, axis=2)
    weights = jnp.exp(scores - new_max[:, :, None])
    shrink = jnp.exp(running_max - new_max)
    denominator = denominator * shrink + jnp.sum(weights, axis=2)
    weighted = weighted * shrink[:, :, None] + jnp.einsum(
        "qhk,khd->qhd",
        weights.astype(jnp.bfloat16),
        value_heads,
        preferred_element_type=jnp.float32,
    )
    return (new_max, denominator, weighted)


def initial_state(row_count, head_count):
    return (
        jnp.full((row_count, head_count), -jnp.inf, jnp.float32),
        jnp.zeros((row_count, head_count), jnp.float32),
        jnp.zeros((row_count, head_count, HEAD), jnp.float32),
    )


def on_device(query, keys, values, out_weight, out_gain):
    grouped_q, grouped_k, grouped_v = (
        lax.all_to_all(query, "uly", split_axis=1, concat_axis=0, tiled=True),
        lax.all_to_all(keys, "uly", split_axis=1, concat_axis=0, tiled=True),
        lax.all_to_all(values, "uly", split_axis=1, concat_axis=0, tiled=True),
    )
    row_count = grouped_q.shape[0]
    features = grouped_q.shape[1]
    local_heads = features // HEAD
    query_heads = grouped_q.reshape(row_count, local_heads, HEAD)
    half_heads = local_heads // 2
    half_width = half_heads * HEAD
    low_state = make_fold(
        query_heads[:, :half_heads],
        initial_state(row_count, half_heads),
        (
            lax.all_gather(grouped_k[:, :half_width], "blk", axis=0, tiled=True),
            lax.all_gather(grouped_v[:, :half_width], "blk", axis=0, tiled=True),
        ),
    )
    high_state = make_fold(
        query_heads[:, half_heads:],
        initial_state(row_count, local_heads - half_heads),
        (
            lax.all_gather(grouped_k[:, half_width:], "blk", axis=0, tiled=True),
            lax.all_gather(grouped_v[:, half_width:], "blk", axis=0, tiled=True),
        ),
    )
    denominator = jnp.concatenate([low_state[1], high_state[1]], axis=1)
    weighted = jnp.concatenate([low_state[2], high_state[2]], axis=1)
    attended = (
        (weighted / denominator[:, :, None]).reshape(row_count, features).astype(jnp.bfloat16)
    )
    partial_value = jnp.dot(
        attended,
        lax.all_gather(out_weight, "blk", axis=1, tiled=True),
        preferred_element_type=jnp.float32,
    )
    summed = lax.psum_scatter(
        partial_value.astype(jnp.bfloat16), "uly", scatter_dimension=0, tiled=True
    ).astype(jnp.float32)
    return (out_gain * summed).astype(jnp.bfloat16)


def attend_kernel(
    nb, nu,
    q_hbm, k_hbm, v_hbm, w_hbm, gain_ref, out_ref,
    q_ref, k_ref, v_ref, stage_a, stage_b, got_a, got_b, w_ref,
    att_pair, att_one, att_all, part_f32, part_send, part_got, final_send,
    in_sem, send_a, send_b, recv_a, recv_b,
    send_p, recv_p, send_o, recv_o, pass_p, pass_o, send_r, recv_r, send_f, recv_f,
):
    n = nb * nu
    rows, width = q_ref.shape
    tokens = n * rows
    pairs = stage_a.shape[1] // 3
    heads = 2 * pairs + 1
    block = nu * rows
    half = block // 2
    side = nb // 2
    upper = (rows // 8 + 1) // 2 * 8
    order = sorted(range(nb), key=lambda t: -abs(2 * t - nb + 1))
    scale = 1.0 / math.sqrt(HEAD)
    me_b, me_u = lax.axis_index("blk"), lax.axis_index("uly")
    me = me_b * nu + me_u
    my_side = me_b // side
    gate_here = (side - 1) + my_side
    gate_there = side - my_side
    is_gate = me_b == gate_here

    def there(b, u):
        return dict(device_id={"blk": b, "uly": u}, device_id_type=MESH)

    barrier = pltpu.get_barrier_semaphore()

    @pl.loop(1, n)
    def _(d):
        j = lax.rem(me + d, n)
        pl.semaphore_signal(barrier, inc=1, **there(j // nu, lax.rem(j, nu)))

    loads = [
        pltpu.make_async_copy(src, dst, in_sem.at[i])
        for i, (src, dst) in enumerate(
            ((q_hbm, q_ref), (k_hbm, k_ref), (v_hbm, v_ref), (w_hbm, w_ref)))
    ]
    for load in loads:
        load.start()
    for load in loads[:3]:
        load.wait()

    for c in range(n):
        odd = c % 2
        first = (heads * c - odd) // 2
        pair_at = first + odd
        one_at = first + (0 if odd else pairs)
        for s, ref in enumerate((q_ref, k_ref, v_ref)):
            for p in range(pairs):
                stage_a[c, s * pairs + p] = ref[:, pl.ds((pair_at + p) * LANES, LANES)]
        q_one, k_one, v_one = (
            ref[:, pl.ds(one_at * LANES, LANES)].astype(jnp.float32)[:, odd * HEAD:(odd + 1) * HEAD]
            for ref in (q_ref, k_ref, v_ref))
        rest = jnp.concatenate(
            [v_one[upper:], jnp.zeros((2 * upper - rows, HEAD), jnp.float32)]
            if 2 * upper > rows else [v_one[upper:]], axis=0)
        stage_b[c] = jnp.concatenate(
            [jnp.concatenate([q_one, k_one], axis=1), jnp.concatenate([v_one[:upper], rest], axis=1)],
            axis=0).astype(jnp.bfloat16)
    mine = me_u * nb + me_b
    got_a[me] = stage_a[mine]
    got_b[me] = stage_b[mine]

    pl.semaphore_wait(barrier, n - 1)

    def exchange(stage, got, send, recv, d):
        j = lax.rem(me + d, n)
        b, u = j // nu, lax.rem(j, nu)
        return pltpu.make_async_remote_copy(
            src_ref=stage.at[u * nb + b], dst_ref=got.at[me],
            send_sem=send.at[d], recv_sem=recv.at[me], **there(b, u))

    def arrival(stage, got, send, recv, d):
        j = lax.rem(me + n - d, n)
        return pltpu.make_async_remote_copy(
            src_ref=stage.at[j], dst_ref=got.at[j],
            send_sem=send.at[d], recv_sem=recv.at[j], **there(me_b, me_u))

    a_refs = (stage_a, got_a, send_a, recv_a)
    b_refs = (stage_b, got_b, send_b, recv_b)

    @pl.loop(1, n)
    def _(d):
        exchange(*a_refs, d).start()

    @pl.loop(1, n)
    def _(d):
        exchange(*b_refs, d).start()

    @pl.loop(1, n)
    def _(d):
        arrival(*a_refs, d).wait_recv()

    def softmax(scores):
        scores = scores * scale
        top = jnp.max(scores, axis=1, keepdims=True)
        weights = jnp.exp(scores - top)
        return weights.astype(jnp.bfloat16), jnp.sum(weights, axis=1, keepdims=True)

    def against(a, b):
        return lax.dot_general(a, b, (((1,), (1,)), ((), ())), preferred_element_type=jnp.float32)

    wide_low = lax.broadcasted_iota(jnp.int32, (tokens, LANES), 1) < HEAD

    def whole(ref, s):
        return jnp.concatenate([ref[i, s].astype(jnp.float32) for i in range(n)], axis=0)

    for p in range(pairs):
        q_all = whole(got_a, p)
        k_all = whole(got_a, pairs + p).astype(jnp.bfloat16)
        v_all = whole(got_a, 2 * pairs + p).astype(jnp.bfloat16)
        pieces = []
        for keep in (wide_low, jnp.logical_not(wide_low)):
            q_one = jnp.where(keep, q_all, 0.0).astype(jnp.bfloat16)
            weights, total = softmax(against(q_one, k_all))
            pieces.append(jnp.dot(weights, v_all, preferred_element_type=jnp.float32) / total)
        joined = jnp.where(wide_low, *pieces).astype(jnp.bfloat16)
        for t in range(nb):
            att_pair[me_b, t, p] = joined[t * block:(t + 1) * block]

    def target(d):
        return gate_there if d == 0 else my_side * side + lax.rem(me_b + d, side)

    def spread(ref, send, recv, d, t):
        return pltpu.make_async_remote_copy(
            src_ref=ref.at[me_b, t], dst_ref=ref.at[me_b, t],
            send_sem=send.at[d, t], recv_sem=recv.at[me_b, t], **there(target(d), me_u))

    def spread_in(ref, send, recv, b, t):
        return pltpu.make_async_remote_copy(
            src_ref=ref.at[b, t], dst_ref=ref.at[b, t],
            send_sem=send.at[0, t], recv_sem=recv.at[b, t], **there(me_b, me_u))

    def pass_on(ref, sems, recv, d, far, t):
        return pltpu.make_async_remote_copy(
            src_ref=ref.at[far, t], dst_ref=ref.at[far, t],
            send_sem=sems.at[d, far, t], recv_sem=recv.at[far, t], **there(target(d), me_u))

    pair_refs, one_refs = (att_pair, send_p, recv_p), (att_one, send_o, recv_o)
    early = order[:side]
    for t in early:
        for d in range(side):
            spread(*pair_refs, d, t).start()

    @pl.loop(1, n)
    def _(d):
        arrival(*b_refs, d).wait_recv()

    got = [got_b[i].astype(jnp.float32) for i in range(n)]
    qk_all = jnp.concatenate([g[:rows] for g in got], axis=0)
    v_all = jnp.concatenate(
        [piece for g in got
         for piece in (g[rows:, :HEAD], g[rows:2 * rows - upper, HEAD:])], axis=0)
    weights, total = softmax(
        against(qk_all[:, :HEAD].astype(jnp.bfloat16), qk_all[:, HEAD:].astype(jnp.bfloat16)))
    single = jnp.dot(
        weights, v_all.astype(jnp.bfloat16), preferred_element_type=jnp.float32) / total
    for t in range(nb):
        at = t * block
        att_one[me_b, t] = jnp.concatenate(
            [single[at:at + half], single[at + half:at + block]], axis=1).astype(jnp.bfloat16)
    for t in order:
        for d in range(side):
            if t not in early:
                spread(*pair_refs, d, t).start()
            spread(*one_refs, d, t).start()

    def scatter(to, d):
        u = lax.rem(me_u + d, nu)
        return pltpu.make_async_remote_copy(
            src_ref=part_send.at[to, u], dst_ref=part_got.at[to, me_u],
            send_sem=send_r.at[to, d], recv_sem=recv_r.at[to, me_u], **there(me_b, u))

    def scatter_in(to, d):
        u = lax.rem(me_u + nu - d, nu)
        return pltpu.make_async_remote_copy(
            src_ref=part_send.at[to, u], dst_ref=part_got.at[to, u],
            send_sem=send_r.at[to, d], recv_sem=recv_r.at[to, u], **there(me_b, me_u))

    def final(to):
        return pltpu.make_async_remote_copy(
            src_ref=final_send.at[to], dst_ref=out_ref.at[me_b],
            send_sem=send_f.at[to], recv_sem=recv_f.at[me_b], **there(to, me_u))

    def final_in(d):
        b = lax.rem(me_b + nb - d, nb)
        return pltpu.make_async_remote_copy(
            src_ref=final_send.at[b], dst_ref=out_ref.at[b],
            send_sem=send_f.at[b], recv_sem=recv_f.at[b], **there(me_b, me_u))

    def reduce(to):
        total = part_f32[to, me_u]
        for d in range(1, nu):
            scatter_in(to, d).wait_recv()
            total += part_got[to, lax.rem(me_u + nu - d, nu)].astype(jnp.float32)
        gated = (gain_ref[me_b] * total).astype(jnp.bfloat16)

        @pl.when(me_b == to)
        def _():
            out_ref[to] = gated

        @pl.when(me_b != to)
        def _():
            final_send[to] = gated
            final(to).start()

    loads[3].wait()
    far_side = (1 - my_side) * side
    for turn, t in enumerate(order):
        for refs, sems in ((pair_refs, pass_p), (one_refs, pass_o)):
            for i in range(side):
                far = far_side + i
                spread_in(*refs, far, t).wait_recv()

                @pl.when(is_gate)
                def _():
                    for d in range(1, side):
                        pass_on(refs[0], sems, refs[2], d, far, t).start()
        for d in range(1, side):
            near = target(d)
            spread_in(*pair_refs, near, t).wait_recv()
            spread_in(*one_refs, near, t).wait_recv()
        for b in range(0, nb, 2):
            tile = heads * b // 2
            for p in range(pairs):
                att_all[:, pl.ds((tile + p) * LANES, LANES)] = att_pair[b, t, p]
                att_all[:, pl.ds((tile + pairs + 1 + p) * LANES, LANES)] = att_pair[b + 1, t, p]
            even, odd = att_one[b, t].astype(jnp.float32), att_one[b + 1, t].astype(jnp.float32)
            at = pl.ds((tile + pairs) * LANES, LANES)
            att_all[:, at] = jnp.concatenate(
                [jnp.concatenate([even[:, :HEAD], odd[:, :HEAD]], axis=1),
                 jnp.concatenate([even[:, HEAD:], odd[:, HEAD:]], axis=1)],
                axis=0).astype(jnp.bfloat16)
        part = jnp.dot(att_all[...], w_ref[...], preferred_element_type=jnp.float32)
        for u in range(nu):
            one = part[u * rows:(u + 1) * rows]
            part_f32[t, u] = one
            part_send[t, u] = one.astype(jnp.bfloat16)
        for d in range(1, nu):
            scatter(t, d).start()
        if turn >= 2:
            reduce(order[turn - 2])
    for t in order[-2:]:
        reduce(t)

    for d in range(1, nb):
        final_in(d).wait_recv()

    @pl.loop(1, n)
    def _(d):
        exchange(*a_refs, d).wait_send()
        exchange(*b_refs, d).wait_send()

    for t in range(nb):
        for d in range(side):
            spread(*pair_refs, d, t).wait_send()
            spread(*one_refs, d, t).wait_send()
        for d in range(1, nu):
            scatter(t, d).wait_send()

        @pl.when(me_b != t)
        def _():
            final(t).wait_send()

        @pl.when(is_gate)
        def _():
            for i in range(side):
                for d in range(1, side):
                    pass_on(att_pair, pass_p, recv_p, d, far_side + i, t).wait_send()
                    pass_on(att_one, pass_o, recv_o, d, far_side + i, t).wait_send()


def fused(nb, nu, query, keys, values, out_weight, out_gain):
    n = nb * nu
    rows, width = query.shape
    heads = width // HEAD // n
    pairs = heads // 2
    depth, columns = out_weight.shape
    bf16, f32 = jnp.bfloat16, jnp.float32
    vmem, dma = pltpu.VMEM, pltpu.SemaphoreType.DMA
    in_vmem = pl.BlockSpec(memory_space=pltpu.VMEM)
    in_place = pl.BlockSpec(memory_space=pl.ANY)
    block, side = nu * rows, nb // 2
    upper = (rows // 8 + 1) // 2 * 8
    gathered = pl.pallas_call(
        functools.partial(attend_kernel, nb, nu),
        out_shape=jax.ShapeDtypeStruct((nb, rows, columns), bf16),
        in_specs=[in_place, in_place, in_place, in_place, in_vmem],
        out_specs=in_vmem,
        scratch_shapes=[
            vmem((rows, width), bf16), vmem((rows, width), bf16), vmem((rows, width), bf16),
            vmem((n, 3 * pairs, rows, LANES), bf16),
            vmem((n, rows + upper, LANES), bf16),
            vmem((n, 3 * pairs, rows, LANES), bf16),
            vmem((n, rows + upper, LANES), bf16),
            vmem((depth, columns), bf16),
            vmem((nb, nb, pairs, block, LANES), bf16),
            vmem((nb, nb, block // 2, LANES), bf16),
            vmem((block, depth), bf16),
            vmem((nb, nu, rows, columns), f32),
            vmem((nb, nu, rows, columns), bf16),
            vmem((nb, nu, rows, columns), bf16),
            vmem((nb, rows, columns), bf16),
            dma((4,)), dma((n,)), dma((n,)), dma((n,)), dma((n,)),
            dma((side, nb)), dma((nb, nb)), dma((side, nb)), dma((nb, nb)),
            dma((side, nb, nb)), dma((side, nb, nb)),
            dma((nb, nu)), dma((nb, nu)), dma((nb,)), dma((nb,)),
        ],
        compiler_params=pltpu.CompilerParams(collective_id=0, has_side_effects=True),
    )(query, keys, values, out_weight, out_gain.reshape(nb, 1, columns))
    return gathered.transpose(1, 0, 2).reshape(rows, width)


def on_any(nb, nu, query, keys, values, out_weight, out_gain):
    n = nb * nu
    rows, width = query.shape
    heads = width // HEAD
    suits = (
        heads % n == 0 and (heads // n) % 2 == 1 and heads // n > 1 and nb % 2 == 0
        and rows % 8 == 0 and (width // nb) % LANES == 0
    )
    plan = functools.partial(fused, nb, nu) if suits else on_device
    return plan(query, keys, values, out_weight, out_gain)


def solution(mesh):
    in_specs = (
        P(("group", "blk", "uly"), None),
        P(("group", "blk", "uly"), None),
        P(("group", "blk", "uly"), None),
        P("uly", "blk"),
        P(),
    )
    out_specs = P(("group", "blk", "uly"), None)
    body = functools.partial(on_any, mesh.shape["blk"], mesh.shape["uly"])
    return jax.shard_map(
        body, mesh=mesh, in_specs=in_specs, out_specs=out_specs, check_vma=False
    )
```

```python
import functools
import math

import jax
import jax.numpy as jnp
from jax import lax
from jax.experimental import pallas as pl
from jax.experimental.pallas import tpu as pltpu
from jax.sharding import PartitionSpec as P

HEAD = 64
LANES = 128
MESH = pl.DeviceIdType.MESH

def make_fold(query_heads, state_now, pieces):
    score_scale = 1.0 / math.sqrt(HEAD)
    head_count = query_heads.shape[1]
    running_max, denominator, weighted = state_now
    key_part, value_part = pieces
    key_count = key_part.shape[0]
    key_heads = key_part.reshape(key_count, head_count, HEAD)
    value_heads = value_part.reshape(key_count, head_count, HEAD)
    scores = (
        jnp.einsum("qhd,khd->qhk", query_heads, key_heads, preferred_element_type=jnp.float32)
        * score_scale
    )
    new_max = jnp.max(scores, axis=2)
    weights = jnp.exp(scores - new_max[:, :, None])
    shrink = jnp.exp(running_max - new_max)
    denominator = denominator * shrink + jnp.sum(weights, axis=2)
    weighted = weighted * shrink[:, :, None] + jnp.einsum(
        "qhk,khd->qhd",
        weights.astype(jnp.bfloat16),
        value_heads,
        preferred_element_type=jnp.float32,
    )
    return (new_max, denominator, weighted)


def initial_state(row_count, head_count):
    return (
        jnp.full((row_count, head_count), -jnp.inf, jnp.float32),
        jnp.zeros((row_count, head_count), jnp.float32),
        jnp.zeros((row_count, head_count, HEAD), jnp.float32),
    )


def on_device(query, keys, values, out_weight, out_gain):
    grouped_q, grouped_k, grouped_v = (
        lax.all_to_all(query, "uly", split_axis=1, concat_axis=0, tiled=True),
        lax.all_to_all(keys, "uly", split_axis=1, concat_axis=0, tiled=True),
        lax.all_to_all(values, "uly", split_axis=1, concat_axis=0, tiled=True),
    )
    row_count = grouped_q.shape[0]
    features = grouped_q.shape[1]
    local_heads = features // HEAD
    query_heads = grouped_q.reshape(row_count, local_heads, HEAD)
    half_heads = local_heads // 2
    half_width = half_heads * HEAD
    low_state = make_fold(
        query_heads[:, :half_heads],
        initial_state(row_count, half_heads),
        (
            lax.all_gather(grouped_k[:, :half_width], "blk", axis=0, tiled=True),
            lax.all_gather(grouped_v[:, :half_width], "blk", axis=0, tiled=True),
        ),
    )
    high_state = make_fold(
        query_heads[:, half_heads:],
        initial_state(row_count, local_heads - half_heads),
        (
            lax.all_gather(grouped_k[:, half_width:], "blk", axis=0, tiled=True),
            lax.all_gather(grouped_v[:, half_width:], "blk", axis=0, tiled=True),
        ),
    )
    denominator = jnp.concatenate([low_state[1], high_state[1]], axis=1)
    weighted = jnp.concatenate([low_state[2], high_state[2]], axis=1)
    attended = (
        (weighted / denominator[:, :, None]).reshape(row_count, features).astype(jnp.bfloat16)
    )
    partial_value = jnp.dot(
        attended,
        lax.all_gather(out_weight, "blk", axis=1, tiled=True),
        preferred_element_type=jnp.float32,
    )
    summed = lax.psum_scatter(
        partial_value.astype(jnp.bfloat16), "uly", scatter_dimension=0, tiled=True
    ).astype(jnp.float32)
    return (out_gain * summed).astype(jnp.bfloat16)


def attend_kernel(
    nb, nu,
    q_hbm, k_hbm, v_hbm, w_hbm, gain_ref, out_ref,
    q_ref, k_ref, v_ref, stage_a, stage_b, got_a, got_b, w_ref,
    att_pair, att_one, att_all, part_f32, part_send, part_got, final_send,
    in_sem, send_a, send_b, recv_a, recv_b,
    send_p, recv_p, send_o, recv_o, pass_p, pass_o, send_r, recv_r, send_f, recv_f,
):
    n = nb * nu
    rows, width = q_ref.shape
    tokens = n * rows
    pairs = stage_a.shape[1] // 3
    heads = 2 * pairs + 1
    block = nu * rows
    half = block // 2
    side = nb // 2
    upper = (rows // 8 + 1) // 2 * 8
    scale = 1.0 / math.sqrt(HEAD)
    me_b, me_u = lax.axis_index("blk"), lax.axis_index("uly")
    me = me_b * nu + me_u
    my_side = me_b // side
    gate_here = (side - 1) + my_side
    gate_there = side - my_side
    is_gate = me_b == gate_here

    def turn_of(b, e):
        upward = b // side
        return upward * e + (1 - upward) * (nb - 1 - e)

    def there(b, u):
        return dict(device_id={"blk": b, "uly": u}, device_id_type=MESH)

    barrier = pltpu.get_barrier_semaphore()

    @pl.loop(1, n)
    def _(d):
        j = lax.rem(me + d, n)
        pl.semaphore_signal(barrier, inc=1, **there(j // nu, lax.rem(j, nu)))

    loads = [
        pltpu.make_async_copy(src, dst, in_sem.at[i])
        for i, (src, dst) in enumerate(
            ((q_hbm, q_ref), (k_hbm, k_ref), (v_hbm, v_ref), (w_hbm, w_ref)))
    ]
    for load in loads:
        load.start()
    for load in loads[:3]:
        load.wait()

    for c in range(n):
        odd = c % 2
        first = (heads * c - odd) // 2
        pair_at = first + odd
        one_at = first + (0 if odd else pairs)
        for s, ref in enumerate((q_ref, k_ref, v_ref)):
            for p in range(pairs):
                stage_a[c, s * pairs + p] = ref[:, pl.ds((pair_at + p) * LANES, LANES)]
        q_one, k_one, v_one = (
            ref[:, pl.ds(one_at * LANES, LANES)].astype(jnp.float32)[:, odd * HEAD:(odd + 1) * HEAD]
            for ref in (q_ref, k_ref, v_ref))
        rest = jnp.concatenate(
            [v_one[upper:], jnp.zeros((2 * upper - rows, HEAD), jnp.float32)]
            if 2 * upper > rows else [v_one[upper:]], axis=0)
        stage_b[c] = jnp.concatenate(
            [jnp.concatenate([q_one, k_one], axis=1), jnp.concatenate([v_one[:upper], rest], axis=1)],
            axis=0).astype(jnp.bfloat16)
    mine = me_u * nb + me_b
    got_a[me] = stage_a[mine]
    got_b[me] = stage_b[mine]

    pl.semaphore_wait(barrier, n - 1)

    def exchange(stage, got, send, recv, b, u):
        return pltpu.make_async_remote_copy(
            src_ref=stage.at[u * nb + b], dst_ref=got.at[me],
            send_sem=send.at[b * nu + u], recv_sem=recv.at[me], **there(b, u))

    def arrival(stage, got, send, recv, d):
        j = lax.rem(me + n - d, n)
        return pltpu.make_async_remote_copy(
            src_ref=stage.at[j], dst_ref=got.at[j],
            send_sem=send.at[j], recv_sem=recv.at[j], **there(me_b, me_u))

    a_refs = (stage_a, got_a, send_a, recv_a)
    b_refs = (stage_b, got_b, send_b, recv_b)

    for refs in (a_refs, b_refs):
        for d in range(1, n):
            j = lax.rem(me_b + d // nu, nb) * nu + lax.rem(me_u + d % nu, nu)
            exchange(*refs, j // nu, lax.rem(j, nu)).start()

    @pl.loop(1, n)
    def _(d):
        arrival(*a_refs, d).wait_recv()

    def softmax(scores):
        scores = scores * scale
        top = jnp.max(scores, axis=1, keepdims=True)
        weights = jnp.exp(scores - top)
        return weights.astype(jnp.bfloat16), jnp.sum(weights, axis=1, keepdims=True)

    def against(a, b):
        return lax.dot_general(a, b, (((1,), (1,)), ((), ())), preferred_element_type=jnp.float32)

    wide_low = lax.broadcasted_iota(jnp.int32, (tokens, LANES), 1) < HEAD

    def whole(ref, s):
        return jnp.concatenate([ref[i, s].astype(jnp.float32) for i in range(n)], axis=0)

    for p in range(pairs):
        q_all = whole(got_a, p)
        k_all = whole(got_a, pairs + p).astype(jnp.bfloat16)
        v_all = whole(got_a, 2 * pairs + p).astype(jnp.bfloat16)
        pieces = []
        for keep in (wide_low, jnp.logical_not(wide_low)):
            q_one = jnp.where(keep, q_all, 0.0).astype(jnp.bfloat16)
            weights, total = softmax(against(q_one, k_all))
            pieces.append(jnp.dot(weights, v_all, preferred_element_type=jnp.float32) / total)
        joined = jnp.where(wide_low, *pieces).astype(jnp.bfloat16)
        for t in range(nb):
            att_pair[me_b, t, p] = joined[t * block:(t + 1) * block]

    def target(d):
        return gate_there if d == 0 else my_side * side + lax.rem(me_b + d, side)

    def spread(ref, send, recv, d, e):
        t = turn_of(target(d), e)
        return pltpu.make_async_remote_copy(
            src_ref=ref.at[me_b, t], dst_ref=ref.at[me_b, t],
            send_sem=send.at[d, t], recv_sem=recv.at[me_b, t], **there(target(d), me_u))

    def spread_in(ref, send, recv, b, t):
        return pltpu.make_async_remote_copy(
            src_ref=ref.at[b, t], dst_ref=ref.at[b, t],
            send_sem=send.at[0, t], recv_sem=recv.at[b, t], **there(me_b, me_u))

    def pass_on(ref, sems, recv, d, far, t):
        return pltpu.make_async_remote_copy(
            src_ref=ref.at[far, t], dst_ref=ref.at[far, t],
            send_sem=sems.at[d, far, t], recv_sem=recv.at[far, t], **there(target(d), me_u))

    pair_refs, one_refs = (att_pair, send_p, recv_p), (att_one, send_o, recv_o)
    plan = [(0, e) for e in range(side)] + [(1, e) for e in range(side)]
    plan += [(kind, e) for e in range(side, nb) for kind in (0, 1)]
    both = ((*pair_refs, pass_p), (*one_refs, pass_o))
    for kind, e in plan[:side]:
        for d in range(side):
            spread(*both[kind][:3], d, e).start()

    @pl.loop(1, n)
    def _(d):
        arrival(*b_refs, d).wait_recv()

    got = [got_b[i].astype(jnp.float32) for i in range(n)]
    qk_all = jnp.concatenate([g[:rows] for g in got], axis=0)
    v_all = jnp.concatenate(
        [piece for g in got
         for piece in (g[rows:, :HEAD], g[rows:2 * rows - upper, HEAD:])], axis=0)
    weights, total = softmax(
        against(qk_all[:, :HEAD].astype(jnp.bfloat16), qk_all[:, HEAD:].astype(jnp.bfloat16)))
    single = jnp.dot(
        weights, v_all.astype(jnp.bfloat16), preferred_element_type=jnp.float32) / total
    for t in range(nb):
        at = t * block
        att_one[me_b, t] = jnp.concatenate(
            [single[at:at + half], single[at + half:at + block]], axis=1).astype(jnp.bfloat16)
    for kind, e in plan[side:]:
        for d in range(side):
            spread(*both[kind][:3], d, e).start()

    def scatter(to, d):
        u = lax.rem(me_u + d, nu)
        return pltpu.make_async_remote_copy(
            src_ref=part_send.at[to, u], dst_ref=part_got.at[to, me_u],
            send_sem=send_r.at[to, d], recv_sem=recv_r.at[to, me_u], **there(me_b, u))

    def scatter_in(to, d):
        u = lax.rem(me_u + nu - d, nu)
        return pltpu.make_async_remote_copy(
            src_ref=part_send.at[to, u], dst_ref=part_got.at[to, u],
            send_sem=send_r.at[to, d], recv_sem=recv_r.at[to, u], **there(me_b, me_u))

    def final(to):
        return pltpu.make_async_remote_copy(
            src_ref=final_send.at[to], dst_ref=out_ref.at[me_b],
            send_sem=send_f.at[to], recv_sem=recv_f.at[me_b], **there(to, me_u))

    def final_in(d):
        b = lax.rem(me_b + nb - d, nb)
        return pltpu.make_async_remote_copy(
            src_ref=final_send.at[b], dst_ref=out_ref.at[b],
            send_sem=send_f.at[b], recv_sem=recv_f.at[b], **there(me_b, me_u))

    def reduce(e):
        to = turn_of(me_b, e)
        total = part_f32[to, me_u]
        for d in range(1, nu):
            scatter_in(to, d).wait_recv()
            total += part_got[to, lax.rem(me_u + nu - d, nu)].astype(jnp.float32)
        gated = (gain_ref[me_b] * total).astype(jnp.bfloat16)

        @pl.when(me_b == to)
        def _():
            out_ref[to] = gated

        @pl.when(me_b != to)
        def _():
            final_send[to] = gated
            final(to).start()

    loads[3].wait()
    far_side = (1 - my_side) * side
    for kind, turn in plan:
        t = turn_of(me_b, turn)
        ref, send, recv, passed = both[kind]
        for i in range(side):
            far = far_side + i
            spread_in(ref, send, recv, far, t).wait_recv()

            @pl.when(is_gate)
            def _():
                for d in range(1, side):
                    pass_on(ref, passed, recv, d, far, t).start()
        if kind == 0:
            continue
        for d in range(1, side):
            near = target(d)
            spread_in(*pair_refs, near, t).wait_recv()
            spread_in(*one_refs, near, t).wait_recv()
        for b in range(0, nb, 2):
            tile = heads * b // 2
            for p in range(pairs):
                att_all[:, pl.ds((tile + p) * LANES, LANES)] = att_pair[b, t, p]
                att_all[:, pl.ds((tile + pairs + 1 + p) * LANES, LANES)] = att_pair[b + 1, t, p]
            even, odd = att_one[b, t].astype(jnp.float32), att_one[b + 1, t].astype(jnp.float32)
            at = pl.ds((tile + pairs) * LANES, LANES)
            att_all[:, at] = jnp.concatenate(
                [jnp.concatenate([even[:, :HEAD], odd[:, :HEAD]], axis=1),
                 jnp.concatenate([even[:, HEAD:], odd[:, HEAD:]], axis=1)],
                axis=0).astype(jnp.bfloat16)
        part = jnp.dot(att_all[...], w_ref[...], preferred_element_type=jnp.float32)
        for u in range(nu):
            one = part[u * rows:(u + 1) * rows]
            part_f32[t, u] = one
            part_send[t, u] = one.astype(jnp.bfloat16)
        for d in range(1, nu):
            scatter(t, d).start()
        if turn >= 2:
            reduce(turn - 2)
    for turn in range(nb - 2, nb):
        reduce(turn)

    for d in range(1, nb):
        final_in(d).wait_recv()

    @pl.loop(1, n)
    def _(d):
        j = lax.rem(me + d, n)
        exchange(*a_refs, j // nu, lax.rem(j, nu)).wait_send()
        exchange(*b_refs, j // nu, lax.rem(j, nu)).wait_send()

    for t in range(nb):
        for d in range(side):
            spread(*pair_refs, d, t).wait_send()
            spread(*one_refs, d, t).wait_send()
        for d in range(1, nu):
            scatter(t, d).wait_send()

        @pl.when(me_b != t)
        def _():
            final(t).wait_send()

        @pl.when(is_gate)
        def _():
            for i in range(side):
                for d in range(1, side):
                    pass_on(att_pair, pass_p, recv_p, d, far_side + i, t).wait_send()
                    pass_on(att_one, pass_o, recv_o, d, far_side + i, t).wait_send()


def fused(nb, nu, query, keys, values, out_weight, out_gain):
    n = nb * nu
    rows, width = query.shape
    heads = width // HEAD // n
    pairs = heads // 2
    depth, columns = out_weight.shape
    bf16, f32 = jnp.bfloat16, jnp.float32
    vmem, dma = pltpu.VMEM, pltpu.SemaphoreType.DMA
    in_vmem = pl.BlockSpec(memory_space=pltpu.VMEM)
    in_place = pl.BlockSpec(memory_space=pl.ANY)
    block, side = nu * rows, nb // 2
    upper = (rows // 8 + 1) // 2 * 8
    gathered = pl.pallas_call(
        functools.partial(attend_kernel, nb, nu),
        out_shape=jax.ShapeDtypeStruct((nb, rows, columns), bf16),
        in_specs=[in_place, in_place, in_place, in_place, in_vmem],
        out_specs=in_vmem,
        scratch_shapes=[
            vmem((rows, width), bf16), vmem((rows, width), bf16), vmem((rows, width), bf16),
            vmem((n, 3 * pairs, rows, LANES), bf16),
            vmem((n, rows + upper, LANES), bf16),
            vmem((n, 3 * pairs, rows, LANES), bf16),
            vmem((n, rows + upper, LANES), bf16),
            vmem((depth, columns), bf16),
            vmem((nb, nb, pairs, block, LANES), bf16),
            vmem((nb, nb, block // 2, LANES), bf16),
            vmem((block, depth), bf16),
            vmem((nb, nu, rows, columns), f32),
            vmem((nb, nu, rows, columns), bf16),
            vmem((nb, nu, rows, columns), bf16),
            vmem((nb, rows, columns), bf16),
            dma((4,)), dma((n,)), dma((n,)), dma((n,)), dma((n,)),
            dma((side, nb)), dma((nb, nb)), dma((side, nb)), dma((nb, nb)),
            dma((side, nb, nb)), dma((side, nb, nb)),
            dma((nb, nu)), dma((nb, nu)), dma((nb,)), dma((nb,)),
        ],
        compiler_params=pltpu.CompilerParams(collective_id=0, has_side_effects=True),
    )(query, keys, values, out_weight, out_gain.reshape(nb, 1, columns))
    return gathered.transpose(1, 0, 2).reshape(rows, width)


def on_any(nb, nu, query, keys, values, out_weight, out_gain):
    n = nb * nu
    rows, width = query.shape
    heads = width // HEAD
    suits = (
        heads % n == 0 and (heads // n) % 2 == 1 and heads // n > 1 and nb % 2 == 0
        and rows % 8 == 0 and (width // nb) % LANES == 0
    )
    plan = functools.partial(fused, nb, nu) if suits else on_device
    return plan(query, keys, values, out_weight, out_gain)


def solution(mesh):
    in_specs = (
        P(("group", "blk", "uly"), None),
        P(("group", "blk", "uly"), None),
        P(("group", "blk", "uly"), None),
        P("uly", "blk"),
        P(),
    )
    out_specs = P(("group", "blk", "uly"), None)
    body = functools.partial(on_any, mesh.shape["blk"], mesh.shape["uly"])
    return jax.shard_map(
        body, mesh=mesh, in_specs=in_specs, out_specs=out_specs, check_vma=False
    )
```

```python
import functools
import math

import jax
import jax.numpy as jnp
from jax import lax
from jax.experimental import pallas as pl
from jax.experimental.pallas import tpu as pltpu
from jax.sharding import PartitionSpec as P

HEAD = 64
LANES = 128
MESH = pl.DeviceIdType.MESH

def make_fold(query_heads, state_now, pieces):
    score_scale = 1.0 / math.sqrt(HEAD)
    head_count = query_heads.shape[1]
    running_max, denominator, weighted = state_now
    key_part, value_part = pieces
    key_count = key_part.shape[0]
    key_heads = key_part.reshape(key_count, head_count, HEAD)
    value_heads = value_part.reshape(key_count, head_count, HEAD)
    scores = (
        jnp.einsum("qhd,khd->qhk", query_heads, key_heads, preferred_element_type=jnp.float32)
        * score_scale
    )
    new_max = jnp.max(scores, axis=2)
    weights = jnp.exp(scores - new_max[:, :, None])
    shrink = jnp.exp(running_max - new_max)
    denominator = denominator * shrink + jnp.sum(weights, axis=2)
    weighted = weighted * shrink[:, :, None] + jnp.einsum(
        "qhk,khd->qhd",
        weights.astype(jnp.bfloat16),
        value_heads,
        preferred_element_type=jnp.float32,
    )
    return (new_max, denominator, weighted)


def initial_state(row_count, head_count):
    return (
        jnp.full((row_count, head_count), -jnp.inf, jnp.float32),
        jnp.zeros((row_count, head_count), jnp.float32),
        jnp.zeros((row_count, head_count, HEAD), jnp.float32),
    )


def on_device(query, keys, values, out_weight, out_gain):
    grouped_q, grouped_k, grouped_v = (
        lax.all_to_all(query, "uly", split_axis=1, concat_axis=0, tiled=True),
        lax.all_to_all(keys, "uly", split_axis=1, concat_axis=0, tiled=True),
        lax.all_to_all(values, "uly", split_axis=1, concat_axis=0, tiled=True),
    )
    row_count = grouped_q.shape[0]
    features = grouped_q.shape[1]
    local_heads = features // HEAD
    query_heads = grouped_q.reshape(row_count, local_heads, HEAD)
    half_heads = local_heads // 2
    half_width = half_heads * HEAD
    low_state = make_fold(
        query_heads[:, :half_heads],
        initial_state(row_count, half_heads),
        (
            lax.all_gather(grouped_k[:, :half_width], "blk", axis=0, tiled=True),
            lax.all_gather(grouped_v[:, :half_width], "blk", axis=0, tiled=True),
        ),
    )
    high_state = make_fold(
        query_heads[:, half_heads:],
        initial_state(row_count, local_heads - half_heads),
        (
            lax.all_gather(grouped_k[:, half_width:], "blk", axis=0, tiled=True),
            lax.all_gather(grouped_v[:, half_width:], "blk", axis=0, tiled=True),
        ),
    )
    denominator = jnp.concatenate([low_state[1], high_state[1]], axis=1)
    weighted = jnp.concatenate([low_state[2], high_state[2]], axis=1)
    attended = (
        (weighted / denominator[:, :, None]).reshape(row_count, features).astype(jnp.bfloat16)
    )
    partial_value = jnp.dot(
        attended,
        lax.all_gather(out_weight, "blk", axis=1, tiled=True),
        preferred_element_type=jnp.float32,
    )
    summed = lax.psum_scatter(
        partial_value.astype(jnp.bfloat16), "uly", scatter_dimension=0, tiled=True
    ).astype(jnp.float32)
    return (out_gain * summed).astype(jnp.bfloat16)


def attend_kernel(
    nb, nu,
    q_hbm, k_hbm, v_hbm, w_hbm, gain_ref, out_ref,
    q_ref, k_ref, v_ref, stage_a, stage_b, got_a, got_b, w_ref,
    att_pair, att_one, att_all, part_f32, part_send, part_got, final_send,
    in_sem, send_a, send_b, recv_a, recv_b,
    send_p, recv_p, send_o, recv_o, pass_p, pass_o, send_r, recv_r, send_f, recv_f,
):
    n = nb * nu
    rows, width = q_ref.shape
    tokens = n * rows
    pairs = stage_a.shape[1] // 3
    heads = 2 * pairs + 1
    block = nu * rows
    half = block // 2
    side = nb // 2
    upper = (rows // 8 + 1) // 2 * 8
    scale = 1.0 / math.sqrt(HEAD)
    me_b, me_u = lax.axis_index("blk"), lax.axis_index("uly")
    me = me_b * nu + me_u
    my_side = me_b // side
    gate_here = (side - 1) + my_side
    gate_there = side - my_side
    is_gate = me_b == gate_here

    def turn_of(b, e):
        upward = b // side
        return upward * e + (1 - upward) * (nb - 1 - e)

    def there(b, u):
        return dict(device_id={"blk": b, "uly": u}, device_id_type=MESH)

    barrier = pltpu.get_barrier_semaphore()

    @pl.loop(1, n)
    def _(d):
        j = lax.rem(me + d, n)
        pl.semaphore_signal(barrier, inc=1, **there(j // nu, lax.rem(j, nu)))

    loads = [
        pltpu.make_async_copy(src, dst, in_sem.at[i])
        for i, (src, dst) in enumerate(
            ((q_hbm, q_ref), (k_hbm, k_ref), (v_hbm, v_ref), (w_hbm, w_ref)))
    ]
    for load in loads:
        load.start()
    for load in loads[:3]:
        load.wait()

    for c in range(n):
        odd = c % 2
        first = (heads * c - odd) // 2
        pair_at = first + odd
        one_at = first + (0 if odd else pairs)
        for s, ref in enumerate((q_ref, k_ref, v_ref)):
            for p in range(pairs):
                stage_a[c, s * pairs + p] = ref[:, pl.ds((pair_at + p) * LANES, LANES)]
        q_one, k_one, v_one = (
            ref[:, pl.ds(one_at * LANES, LANES)].astype(jnp.float32)[:, odd * HEAD:(odd + 1) * HEAD]
            for ref in (q_ref, k_ref, v_ref))
        rest = jnp.concatenate(
            [v_one[upper:], jnp.zeros((2 * upper - rows, HEAD), jnp.float32)]
            if 2 * upper > rows else [v_one[upper:]], axis=0)
        stage_b[c] = jnp.concatenate(
            [jnp.concatenate([q_one, k_one], axis=1), jnp.concatenate([v_one[:upper], rest], axis=1)],
            axis=0).astype(jnp.bfloat16)
    mine = me_u * nb + me_b
    got_a[me] = stage_a[mine]
    got_b[me] = stage_b[mine]

    pl.semaphore_wait(barrier, n - 1)

    def exchange(stage, got, send, recv, b, u):
        return pltpu.make_async_remote_copy(
            src_ref=stage.at[u * nb + b], dst_ref=got.at[me],
            send_sem=send.at[b * nu + u], recv_sem=recv.at[me], **there(b, u))

    def arrival(stage, got, send, recv, d):
        j = lax.rem(me + n - d, n)
        return pltpu.make_async_remote_copy(
            src_ref=stage.at[j], dst_ref=got.at[j],
            send_sem=send.at[j], recv_sem=recv.at[j], **there(me_b, me_u))

    a_refs = (stage_a, got_a, send_a, recv_a)
    b_refs = (stage_b, got_b, send_b, recv_b)

    for refs in (a_refs, b_refs):
        for d in range(n - 1, 0, -1):
            exchange(*refs, lax.rem(me_b + d // nu, nb), lax.rem(me_u + d % nu, nu)).start()

    @pl.loop(1, n)
    def _(d):
        arrival(*a_refs, d).wait_recv()

    def softmax(scores):
        scores = scores * scale
        top = jnp.max(scores, axis=1, keepdims=True)
        weights = jnp.exp(scores - top)
        return weights.astype(jnp.bfloat16), jnp.sum(weights, axis=1, keepdims=True)

    def against(a, b):
        return lax.dot_general(a, b, (((1,), (1,)), ((), ())), preferred_element_type=jnp.float32)

    wide_low = lax.broadcasted_iota(jnp.int32, (tokens, LANES), 1) < HEAD

    def whole(ref, s):
        return jnp.concatenate([ref[i, s].astype(jnp.float32) for i in range(n)], axis=0)

    for p in range(pairs):
        q_all = whole(got_a, p)
        k_all = whole(got_a, pairs + p).astype(jnp.bfloat16)
        v_all = whole(got_a, 2 * pairs + p).astype(jnp.bfloat16)
        pieces = []
        for keep in (wide_low, jnp.logical_not(wide_low)):
            q_one = jnp.where(keep, q_all, 0.0).astype(jnp.bfloat16)
            weights, total = softmax(against(q_one, k_all))
            pieces.append(jnp.dot(weights, v_all, preferred_element_type=jnp.float32) / total)
        joined = jnp.where(wide_low, *pieces).astype(jnp.bfloat16)
        for t in range(nb):
            att_pair[me_b, t, p] = joined[t * block:(t + 1) * block]

    def target(d):
        return gate_there if d == 0 else my_side * side + lax.rem(me_b + d, side)

    def spread(ref, send, recv, d, e):
        t = turn_of(target(d), e)
        return pltpu.make_async_remote_copy(
            src_ref=ref.at[me_b, t], dst_ref=ref.at[me_b, t],
            send_sem=send.at[d, t], recv_sem=recv.at[me_b, t], **there(target(d), me_u))

    def spread_in(ref, send, recv, b, t):
        return pltpu.make_async_remote_copy(
            src_ref=ref.at[b, t], dst_ref=ref.at[b, t],
            send_sem=send.at[0, t], recv_sem=recv.at[b, t], **there(me_b, me_u))

    def pass_on(ref, sems, recv, d, far, t):
        return pltpu.make_async_remote_copy(
            src_ref=ref.at[far, t], dst_ref=ref.at[far, t],
            send_sem=sems.at[d, far, t], recv_sem=recv.at[far, t], **there(target(d), me_u))

    pair_refs, one_refs = (att_pair, send_p, recv_p), (att_one, send_o, recv_o)
    plan = [(0, e) for e in range(side)] + [(1, e) for e in range(side)]
    plan += [(kind, e) for e in range(side, nb) for kind in (0, 1)]
    both = ((*pair_refs, pass_p), (*one_refs, pass_o))
    for kind, e in plan[:side]:
        for d in range(side):
            spread(*both[kind][:3], d, e).start()

    @pl.loop(1, n)
    def _(d):
        arrival(*b_refs, d).wait_recv()

    got = [got_b[i].astype(jnp.float32) for i in range(n)]
    qk_all = jnp.concatenate([g[:rows] for g in got], axis=0)
    v_all = jnp.concatenate(
        [piece for g in got
         for piece in (g[rows:, :HEAD], g[rows:2 * rows - upper, HEAD:])], axis=0)
    weights, total = softmax(
        against(qk_all[:, :HEAD].astype(jnp.bfloat16), qk_all[:, HEAD:].astype(jnp.bfloat16)))
    single = jnp.dot(
        weights, v_all.astype(jnp.bfloat16), preferred_element_type=jnp.float32) / total
    for t in range(nb):
        at = t * block
        att_one[me_b, t] = jnp.concatenate(
            [single[at:at + half], single[at + half:at + block]], axis=1).astype(jnp.bfloat16)
    for kind, e in plan[side:]:
        for d in range(side):
            spread(*both[kind][:3], d, e).start()

    def scatter(to, d):
        u = lax.rem(me_u + d, nu)
        return pltpu.make_async_remote_copy(
            src_ref=part_send.at[to, u], dst_ref=part_got.at[to, me_u],
            send_sem=send_r.at[to, d], recv_sem=recv_r.at[to, me_u], **there(me_b, u))

    def scatter_in(to, d):
        u = lax.rem(me_u + nu - d, nu)
        return pltpu.make_async_remote_copy(
            src_ref=part_send.at[to, u], dst_ref=part_got.at[to, u],
            send_sem=send_r.at[to, d], recv_sem=recv_r.at[to, u], **there(me_b, me_u))

    def final(to):
        return pltpu.make_async_remote_copy(
            src_ref=final_send.at[to], dst_ref=out_ref.at[me_b],
            send_sem=send_f.at[to], recv_sem=recv_f.at[me_b], **there(to, me_u))

    def final_in(d):
        b = lax.rem(me_b + nb - d, nb)
        return pltpu.make_async_remote_copy(
            src_ref=final_send.at[b], dst_ref=out_ref.at[b],
            send_sem=send_f.at[b], recv_sem=recv_f.at[b], **there(me_b, me_u))

    def reduce(e):
        to = turn_of(me_b, e)
        total = part_f32[to, me_u]
        for d in range(1, nu):
            scatter_in(to, d).wait_recv()
            total += part_got[to, lax.rem(me_u + nu - d, nu)].astype(jnp.float32)
        gated = (gain_ref[me_b] * total).astype(jnp.bfloat16)

        @pl.when(me_b == to)
        def _():
            out_ref[to] = gated

        @pl.when(me_b != to)
        def _():
            final_send[to] = gated
            final(to).start()

    loads[3].wait()
    far_side = (1 - my_side) * side
    for kind, turn in plan:
        t = turn_of(me_b, turn)
        ref, send, recv, passed = both[kind]
        for i in range(side):
            far = far_side + i
            spread_in(ref, send, recv, far, t).wait_recv()

            @pl.when(is_gate)
            def _():
                for d in range(1, side):
                    pass_on(ref, passed, recv, d, far, t).start()
        if kind == 0:
            continue
        for d in range(1, side):
            near = target(d)
            spread_in(*pair_refs, near, t).wait_recv()
            spread_in(*one_refs, near, t).wait_recv()
        for b in range(0, nb, 2):
            tile = heads * b // 2
            for p in range(pairs):
                att_all[:, pl.ds((tile + p) * LANES, LANES)] = att_pair[b, t, p]
                att_all[:, pl.ds((tile + pairs + 1 + p) * LANES, LANES)] = att_pair[b + 1, t, p]
            even, odd = att_one[b, t].astype(jnp.float32), att_one[b + 1, t].astype(jnp.float32)
            at = pl.ds((tile + pairs) * LANES, LANES)
            att_all[:, at] = jnp.concatenate(
                [jnp.concatenate([even[:, :HEAD], odd[:, :HEAD]], axis=1),
                 jnp.concatenate([even[:, HEAD:], odd[:, HEAD:]], axis=1)],
                axis=0).astype(jnp.bfloat16)
        part = jnp.dot(att_all[...], w_ref[...], preferred_element_type=jnp.float32)
        for u in range(nu):
            one = part[u * rows:(u + 1) * rows]
            part_f32[t, u] = one
            part_send[t, u] = one.astype(jnp.bfloat16)
        for d in range(1, nu):
            scatter(t, d).start()
        if turn >= 2:
            reduce(turn - 2)
    for turn in range(nb - 2, nb):
        reduce(turn)

    for d in range(1, nb):
        final_in(d).wait_recv()

    @pl.loop(1, n)
    def _(d):
        j = lax.rem(me + d, n)
        exchange(*a_refs, j // nu, lax.rem(j, nu)).wait_send()
        exchange(*b_refs, j // nu, lax.rem(j, nu)).wait_send()

    for t in range(nb):
        for d in range(side):
            spread(*pair_refs, d, t).wait_send()
            spread(*one_refs, d, t).wait_send()
        for d in range(1, nu):
            scatter(t, d).wait_send()

        @pl.when(me_b != t)
        def _():
            final(t).wait_send()

        @pl.when(is_gate)
        def _():
            for i in range(side):
                for d in range(1, side):
                    pass_on(att_pair, pass_p, recv_p, d, far_side + i, t).wait_send()
                    pass_on(att_one, pass_o, recv_o, d, far_side + i, t).wait_send()


def fused(nb, nu, query, keys, values, out_weight, out_gain):
    n = nb * nu
    rows, width = query.shape
    heads = width // HEAD // n
    pairs = heads // 2
    depth, columns = out_weight.shape
    bf16, f32 = jnp.bfloat16, jnp.float32
    vmem, dma = pltpu.VMEM, pltpu.SemaphoreType.DMA
    in_vmem = pl.BlockSpec(memory_space=pltpu.VMEM)
    in_place = pl.BlockSpec(memory_space=pl.ANY)
    block, side = nu * rows, nb // 2
    upper = (rows // 8 + 1) // 2 * 8
    gathered = pl.pallas_call(
        functools.partial(attend_kernel, nb, nu),
        out_shape=jax.ShapeDtypeStruct((nb, rows, columns), bf16),
        in_specs=[in_place, in_place, in_place, in_place, in_vmem],
        out_specs=in_vmem,
        scratch_shapes=[
            vmem((rows, width), bf16), vmem((rows, width), bf16), vmem((rows, width), bf16),
            vmem((n, 3 * pairs, rows, LANES), bf16),
            vmem((n, rows + upper, LANES), bf16),
            vmem((n, 3 * pairs, rows, LANES), bf16),
            vmem((n, rows + upper, LANES), bf16),
            vmem((depth, columns), bf16),
            vmem((nb, nb, pairs, block, LANES), bf16),
            vmem((nb, nb, block // 2, LANES), bf16),
            vmem((block, depth), bf16),
            vmem((nb, nu, rows, columns), f32),
            vmem((nb, nu, rows, columns), bf16),
            vmem((nb, nu, rows, columns), bf16),
            vmem((nb, rows, columns), bf16),
            dma((4,)), dma((n,)), dma((n,)), dma((n,)), dma((n,)),
            dma((side, nb)), dma((nb, nb)), dma((side, nb)), dma((nb, nb)),
            dma((side, nb, nb)), dma((side, nb, nb)),
            dma((nb, nu)), dma((nb, nu)), dma((nb,)), dma((nb,)),
        ],
        compiler_params=pltpu.CompilerParams(collective_id=0, has_side_effects=True),
    )(query, keys, values, out_weight, out_gain.reshape(nb, 1, columns))
    return gathered.transpose(1, 0, 2).reshape(rows, width)


def on_any(nb, nu, query, keys, values, out_weight, out_gain):
    n = nb * nu
    rows, width = query.shape
    heads = width // HEAD
    suits = (
        heads % n == 0 and (heads // n) % 2 == 1 and heads // n > 1 and nb % 2 == 0
        and rows % 8 == 0 and (width // nb) % LANES == 0
    )
    plan = functools.partial(fused, nb, nu) if suits else on_device
    return plan(query, keys, values, out_weight, out_gain)


def solution(mesh):
    in_specs = (
        P(("group", "blk", "uly"), None),
        P(("group", "blk", "uly"), None),
        P(("group", "blk", "uly"), None),
        P("uly", "blk"),
        P(),
    )
    out_specs = P(("group", "blk", "uly"), None)
    body = functools.partial(on_any, mesh.shape["blk"], mesh.shape["uly"])
    return jax.shard_map(
        body, mesh=mesh, in_specs=in_specs, out_specs=out_specs, check_vma=False
    )
```
